32 devices in a mesh: row: 16 (over z, y, core), col: 2 (over x).
Axes of the slice: x: 2, y: 2, z: 4, core: 2. Of those that a mesh axis runs over, the one named last changes fastest.
Arguments:
- positions: float32 [3, 8192], P(None, ('row', 'col')), as said below
- velocities: float32 [3, 8192], P(None, ('row', 'col')), may hold values from -6 to 6
- old_forces: float32 [3, 8192], P(None, ('row', 'col')), may hold values from -6 to 6
- charges: float32 [8192], P(('row', 'col')), may hold values from -3 to 3
- atom_types: int32 [8192], P(('row', 'col')), may hold values from 0 to 7
- type_table: float32 [7, 8], replicated, may hold values from 0.003 to 2, as said below
- tile_pairs: int32 [16, 2, 2, 32], P('row', 'col'), may hold values from -1 to 31, as said below
Outputs:
- new_positions: float32 [3, 8192], P(None, ('row', 'col'))
- new_velocities: float32 [3, 8192], P(None, ('row', 'col'))
- new_forces: float32 [3, 8192], P(None, ('row', 'col'))
The draws below stay inside these ranges and needn't reach their ends.
Inputs may be any that keep to these rules, and one draw needn't show every extreme that they name: `positions`: the atoms of one block lie together in a cube of its own; the blocks' cubes fill a cubic lattice in the order of the block numbers, at about 0.1 atoms per cubic angstrom. `tile_pairs`: on each device the first n slots hold distinct pairs (a, g) with a below 4 and g below 32, each a tile whose blocks' cubes lie within 12 angstrom of each other; the other slots hold -1 in both entries. n is at most 32, differs from device to device, and equals 32 on the device with the most such tiles when it has 32 or more; the list is a sampled part of each device's near tiles, not all of them. `type_table`: Rows: intrinsic radii 1 to 2, screening scales 0.15 to 0.6, neck weights 0.003 to 0.012, alpha 0.6 to 1, beta 0.3 to 0.9, gamma 0.2 to 0.6, masses 0.5 to 2.
All inputs are finite; a program needn't handle non-finite values.
Results may differ from the reference program's by a relative error of at most 0.0003.
Values sent between devices are 32-bit elements; how exact they have to be, the bound alone decides.
A program may use at most 64 MiB of HBM per device.

```python
import math
import jax
import jax.numpy as jnp
from jax import lax

TILE = 128
BLK_DEV = 2
TILE_CAP = 32
TYPES = 8
ATOMS = 8192
I_BLOCKS = 4
N_ROW = 16
N_COL = 2


def block_frame():
    block_total = ATOMS // TILE
    lattice_side = int(math.ceil(block_total ** (1.0 / 3.0) - 1e-09))
    if lattice_side ** 3 < block_total:
        lattice_side = lattice_side + 1
    cube_edge = (TILE * 10.0) ** (1.0 / 3.0)
    block_ids = jnp.arange(block_total, dtype=jnp.int32)
    lattice = jnp.stack([block_ids // (lattice_side * lattice_side), block_ids // lattice_side % lattice_side, block_ids % lattice_side], axis=0)
    return (lattice.astype(jnp.float32) * cube_edge, cube_edge)


def draw_positions(key, part):
    corners, cube_edge = block_frame()
    unit = jax.random.uniform(jax.random.fold_in(key, 21), (3, ATOMS), jnp.float32)
    return (jnp.repeat(corners, TILE, axis=1) + cube_edge * unit).astype(jnp.float32)


def draw_type_table(key, part):
    lowest = jnp.array([1.0, 0.15, 0.003, 0.6, 0.3, 0.2, 0.5], jnp.float32)[:, None]
    highest = jnp.array([2.0, 0.6, 0.012, 1.0, 0.9, 0.6, 2.0], jnp.float32)[:, None]
    in_logs = jnp.array([1.0, 1.0, 1.0, 0.0, 0.0, 0.0, 1.0], jnp.float32)[:, None]
    unit = jax.random.uniform(jax.random.fold_in(key, 5), (7, TYPES), jnp.float32)
    linear = lowest + (highest - lowest) * unit
    logged = jnp.exp(jnp.log(lowest) + (jnp.log(highest) - jnp.log(lowest)) * unit)
    return (in_logs * logged + (1.0 - in_logs) * linear).astype(jnp.float32)


def draw_tile_pairs(key, part):
    devices_all = N_ROW * N_COL
    i_count = BLK_DEV * N_COL
    j_count = BLK_DEV * N_ROW
    combos = i_count * j_count
    corners, cube_edge = block_frame()
    row_ids = jnp.arange(N_ROW, dtype=jnp.int32)[:, None, None]
    col_ids = jnp.arange(N_COL, dtype=jnp.int32)[None, :, None]
    local_i = jnp.arange(i_count, dtype=jnp.int32)[None, None, :]
    local_j = jnp.arange(j_count, dtype=jnp.int32)[None, None, :]
    global_i = row_ids * i_count + local_i + 0 * col_ids
    global_j = (local_j // BLK_DEV * N_COL + col_ids) * BLK_DEV + local_j % BLK_DEV + 0 * row_ids
    corner_i = jnp.take(corners, global_i.reshape(-1), axis=1).reshape(3, N_ROW, N_COL, i_count)
    corner_j = jnp.take(corners, global_j.reshape(-1), axis=1).reshape(3, N_ROW, N_COL, j_count)
    apart = jnp.abs(corner_i[:, :, :, :, None] - corner_j[:, :, :, None, :])
    gap = jnp.maximum(apart - cube_edge - 0.001, 0.0)
    near = (jnp.sum(gap * gap, axis=0) < 144.0).reshape(devices_all, combos)
    key_list = jax.random.split(jax.random.fold_in(key, 11), devices_all)
    ranks = jax.vmap(lambda subkey: jax.random.permutation(subkey, combos))(key_list).astype(jnp.int32)
    score = jnp.where(near, ranks + 1, 0)
    chosen_score, chosen = lax_top(score)
    near_count = jnp.sum(near.astype(jnp.int32), axis=1)
    fewest = (TILE_CAP + 7) // 8
    level_count = 64
    skew_level = jax.random.randint(jax.random.fold_in(key, 12), (devices_all,), 0, level_count + 1)
    live_count = fewest + (TILE_CAP - fewest) * skew_level * skew_level * skew_level // (level_count * level_count * level_count)
    busiest = jnp.argmax(near_count)
    live_count = jnp.where(jnp.arange(devices_all) == busiest, TILE_CAP, live_count)
    live_count = jnp.minimum(live_count, near_count)
    slot_ids = jnp.arange(TILE_CAP)[None, :]
    live_slot = slot_ids < live_count[:, None]
    first_ids = jnp.where(live_slot, chosen // j_count, -1)
    second_ids = jnp.where(live_slot, chosen % j_count, -1)
    stacked = jnp.stack([first_ids, second_ids], axis=1)
    return stacked.reshape(N_ROW, N_COL, 2, TILE_CAP).astype(jnp.int32)


def lax_top(score):
    return jax.lax.top_k(score, TILE_CAP)


def plant(result, key, smallest, top_value):
    spot = [jax.random.randint(jax.random.fold_in(key, axis), (), 0, length) for axis, length in enumerate(result.shape)]
    longest = result.shape.index(max(result.shape))
    beside = spot[:longest] + [(spot[longest] + 1) % result.shape[longest]] + spot[longest + 1:]
    return result.at[tuple(spot)].set(smallest).at[tuple(beside)].set(top_value)


def levels(key, dims, cuts, least, largest):
    level = 1.0
    for position, blocks in cuts:
        steps = jax.random.uniform(jax.random.fold_in(jax.random.fold_in(key, 6), position), (blocks,), jnp.float32, least / len(cuts), largest / len(cuts))
        level = level * jnp.repeat(jnp.exp(steps), dims[position] // blocks).reshape((-1,) + (1,) * (len(dims) - 1 - position))
    return level


def scatter_about(key, dims, spread, bound, cuts=(), held_as=jnp.bfloat16):
    result = jax.random.normal(key, dims, jnp.float32) * spread
    if len(cuts) > 0:
        result = levels(key, dims, cuts, -0.22, 0.18) * result
    return jnp.clip(result, min=-bound, max=bound).astype(held_as)


def setup_inputs(seed: int = 0) -> dict:
    keys = jax.random.split(jax.random.key(seed), 8)
    return {
        "positions": draw_positions(jax.random.fold_in(keys[7], 71), 0),
        "velocities": scatter_about(keys[1], (3, ATOMS), 1.0, 6.0, ((1, 32),), jnp.float32),
        "old_forces": scatter_about(keys[2], (3, ATOMS), 1.0, 6.0, ((1, 32),), jnp.float32),
        "charges": scatter_about(keys[3], (ATOMS,), 0.5, 3.0, ((0, 32),), jnp.float32),
        "atom_types": plant(jax.random.randint(keys[4], (ATOMS,), 0, TYPES), jax.random.fold_in(keys[4], 1), 0, TYPES - 1).astype(jnp.int32),
        "type_table": draw_type_table(jax.random.fold_in(keys[7], 71), 0),
        "tile_pairs": draw_tile_pairs(jax.random.fold_in(keys[7], 71), 0),
    }


CUTOFF = 12.0
COULOMB = 32.0
TIMESTEP = 0.5
OFFSET = 0.09
NECK_GAP = 0.5
NECK_WIDTH = 16.0

def taper(dist_sq):
    taper_base = jnp.maximum(1.0 - dist_sq / (CUTOFF * CUTOFF), 0.0)
    return (taper_base * taper_base, -2.0 * taper_base / (CUTOFF * CUTOFF))

def screening(dist_sq, intrinsic, other_radius, other_scale, other_neck):
    soft_sq = dist_sq + intrinsic * intrinsic
    neck_gap = intrinsic + other_radius + NECK_GAP
    neck_off = dist_sq - neck_gap * neck_gap
    neck_bump = jnp.exp(-neck_off * neck_off / NECK_WIDTH)
    volume = other_scale * other_radius * other_radius * other_radius
    descreen = volume / (soft_sq * soft_sq) + other_neck * neck_bump
    slope = -2.0 * volume / (soft_sq * soft_sq * soft_sq) - other_neck * neck_bump * neck_off * (2.0 / NECK_WIDTH)
    weight, w_slope = taper(dist_sq)
    return (weight * descreen, w_slope * descreen + weight * slope)

def separation(coords_i, coords_j):
    offset_vec = coords_i[:, :, :, None] - coords_j[:, :, None, :]
    return (offset_vec, lax.optimization_barrier(jnp.sum(offset_vec * offset_vec, axis=1)))

def born_terms(side_i, side_j, mask):
    offset_vec, dist_sq = separation(side_i[:, 0:3], side_j[:, 0:3])
    value, slope = screening(dist_sq, side_i[:, 4][:, :, None], side_j[:, 4][:, None, :], side_j[:, 5][:, None, :], side_j[:, 6][:, None, :])
    return lax.optimization_barrier(jnp.sum(mask * value, axis=2))[:, None, :]

def pair_terms(side_i, side_j, mask):
    offset_vec, dist_sq = separation(side_i[:, 0:3], side_j[:, 0:3])
    charge_pair = side_i[:, 3][:, :, None] * side_j[:, 3][:, None, :]
    radius_j = side_j[:, -1][:, None, :]
    radii_prod = side_i[:, -1][:, :, None] * radius_j
    radii_exp = jnp.exp(-dist_sq / (4.0 * radii_prod))
    inv_eff = 1.0 / jnp.sqrt(dist_sq + radii_prod * radii_exp)
    inv_cube = inv_eff * inv_eff * inv_eff
    weight, w_slope = taper(dist_sq)
    d_dist = mask * charge_pair * (w_slope * inv_eff - 0.5 * weight * (1.0 - 0.25 * radii_exp) * inv_cube)
    d_radius = mask * -0.5 * weight * charge_pair * inv_cube * radii_exp * (1.0 + dist_sq / (4.0 * radii_prod)) * radius_j
    direct = 2.0 * COULOMB * lax.optimization_barrier(jnp.sum(d_dist[:, None] * offset_vec, axis=3))
    return jnp.concatenate([direct, lax.optimization_barrier(jnp.sum(d_radius, axis=2))[:, None, :]], axis=1)

def chain_terms(side_i, side_j, mask):
    offset_vec, dist_sq = separation(side_i[:, 0:3], side_j[:, 0:3])
    value_ij, slope_ij = screening(dist_sq, side_i[:, 4][:, :, None], side_j[:, 4][:, None, :], side_j[:, 5][:, None, :], side_j[:, 6][:, None, :])
    value_ji, slope_ji = screening(dist_sq, side_j[:, 4][:, None, :], side_i[:, 4][:, :, None], side_i[:, 5][:, :, None], side_i[:, 6][:, :, None])
    factor = mask * (side_i[:, -1][:, :, None] * slope_ij + side_j[:, -1][:, None, :] * slope_ji)
    return -2.0 * lax.optimization_barrier(jnp.sum(factor[:, None] * offset_vec, axis=3))

def radius_terms(born_sum, intrinsic, coef_alpha, coef_beta, coef_gamma):
    scaled = intrinsic * born_sum
    poly_arg = coef_alpha * scaled - coef_beta * scaled * scaled + coef_gamma * scaled * scaled * scaled
    squash = jnp.tanh(poly_arg)
    radius = 1.0 / (1.0 / intrinsic - squash / (intrinsic + OFFSET))
    poly_slope = coef_alpha - 2.0 * coef_beta * scaled + 3.0 * coef_gamma * scaled * scaled
    radius_rate = radius * radius * (1.0 - squash * squash) * poly_slope * intrinsic / (intrinsic + OFFSET)
    return (radius, radius_rate)

def reference(positions, velocities, old_forces, charges, atom_types, type_table, tile_pairs):
    type_ids = jnp.arange(TYPES, dtype=jnp.int32)
    onehot = (atom_types[None, :] == type_ids[:, None]).astype(jnp.float32)
    params = lax.optimization_barrier(jnp.sum(type_table[:, :, None] * onehot[None, :, :], axis=1))
    atom_mass = params[6]
    new_positions = positions + TIMESTEP * velocities + TIMESTEP * TIMESTEP / (2.0 * atom_mass) * old_forces
    attrs = jnp.concatenate([new_positions, charges[None, :], params[0:6]], axis=0)
    block_count = ATOMS // TILE
    row_ids = jnp.arange(N_ROW, dtype=jnp.int32)[:, None, None]
    col_ids = jnp.arange(N_COL, dtype=jnp.int32)[None, :, None]
    live_slot = tile_pairs[:, :, 0, :] >= 0
    tiles_i = jnp.maximum(tile_pairs[:, :, 0, :], 0)
    tiles_j = jnp.maximum(tile_pairs[:, :, 1, :], 0)
    block_i = (row_ids * I_BLOCKS + tiles_i).astype(jnp.int32).reshape(-1, TILE_CAP)
    block_j = ((tiles_j // BLK_DEV * N_COL + col_ids) * BLK_DEV + tiles_j % BLK_DEV).astype(jnp.int32).reshape(-1, TILE_CAP)
    live_f = live_slot.astype(jnp.float32).reshape(-1, TILE_CAP)
    diagonal = jnp.eye(TILE, dtype=jnp.float32)

    def all_tiles(func, rows, packed):
        blocks = packed.reshape(packed.shape[0], block_count, TILE)

        def per_device(item):
            list_i, list_j, live_row = item
            side_i = jnp.moveaxis(jnp.take(blocks, list_i, axis=1), 1, 0)
            side_j = jnp.moveaxis(jnp.take(blocks, list_j, axis=1), 1, 0)
            self_pair = (list_i == list_j).astype(jnp.float32)
            mask = live_row[:, None, None] * (1.0 - self_pair[:, None, None] * diagonal)
            return func(side_i, side_j, mask)
        partial_sums = lax.map(per_device, (block_i, block_j, live_f))
        summed = jnp.zeros((block_count, rows, TILE), jnp.float32).at[block_i.reshape(-1)].add(partial_sums.reshape(-1, rows, TILE))
        return jnp.moveaxis(summed, 1, 0).reshape(rows, ATOMS)
    born_part = all_tiles(born_terms, 1, attrs)[0]
    radius, radius_rate = radius_terms(born_part, params[0], params[3], params[4], params[5])
    pair_part = all_tiles(pair_terms, 4, jnp.concatenate([attrs, radius[None, :]], axis=0))
    chain = (COULOMB * charges * charges / (2.0 * radius * radius) - COULOMB * pair_part[3]) * radius_rate
    chain_part = all_tiles(chain_terms, 3, jnp.concatenate([attrs, chain[None, :]], axis=0))
    new_forces = pair_part[0:3] + chain_part
    new_velocities = velocities + TIMESTEP / (2.0 * atom_mass) * (old_forces + new_forces)
    return (new_positions, new_velocities, new_forces)
```

```python
import functools
import math

import jax
import jax.numpy as jnp
from jax import lax
from jax.experimental import pallas as pl
from jax.experimental.pallas import tpu as pltpu
from jax.sharding import PartitionSpec as P

TILE = 128
STRIP = 16
CUTOFF_SQ = 144.0
COULOMB = 32.0
TIMESTEP = 0.5
OFFSET = 0.09
NECK_GAP = 0.5
NECK_WIDTH = 16.0
LOG2E = math.log2(math.e)
MESH = pl.DeviceIdType.MESH
SENT = 5


def kernel(
    rows, cols, blk_dev, table_ref, tiles_ref, pos_ref, vel_ref, frc_ref, chg_ref, typ_ref,
    pos_out, vel_out, frc_out,
    own, recv, attr, total, radius, rate, chain, jcol, geo, mom, acc, part, partial_recv,
    grad_part, grad_recv, frc_part, frc_recv,
    send0, recv0, send1, recv1, send2, recv2, send3, recv3,
):
    my_row, my_col = lax.axis_index("row"), lax.axis_index("col")
    devices = rows * cols
    me = my_row * cols + my_col
    blocks_j, blocks_i = rows * blk_dev, cols * blk_dev
    slots = tiles_ref.shape[1]
    types = table_ref.shape[1]

    barrier = pltpu.get_barrier_semaphore()

    def greet(step, _):
        peer = lax.rem(me + step, devices)
        pl.semaphore_signal(
            barrier, inc=1,
            device_id={"row": lax.div(peer, cols), "col": lax.rem(peer, cols)},
            device_id_type=MESH,
        )
        return 0

    lax.fori_loop(1, devices, greet, 0)

    mass = []
    for b in range(blk_dev):
        span = pl.ds(b * TILE, TILE)
        kind = typ_ref[b : b + 1, :].astype(jnp.float32)
        m = jnp.zeros((1, TILE), jnp.float32)
        for t in range(types):
            m = jnp.where(kind == t, table_ref[6, t], m)
        mass.append(m)
        for k in range(3):
            x = (
                pos_ref[k : k + 1, span]
                + TIMESTEP * vel_ref[k : k + 1, span]
                + TIMESTEP * TIMESTEP / (2.0 * m) * frc_ref[k : k + 1, span]
            )
            pos_out[k : k + 1, span] = x
            own[k * blk_dev + b] = x
            recv[my_row, k * blk_dev + b] = x
            recv[rows + my_col, k * blk_dev + b] = x
        for k, value in ((3, chg_ref[b : b + 1, :]), (4, kind)):
            own[k * blk_dev + b] = value
            recv[my_row, k * blk_dev + b] = value
            recv[rows + my_col, k * blk_dev + b] = value
    acc[...] = jnp.zeros_like(acc)
    attr[...] = jnp.zeros_like(attr)
    total[...] = jnp.zeros_like(total)

    pl.semaphore_wait(barrier, devices - 1)

    def copy0_row(step):
        return pltpu.make_async_remote_copy(
            own, recv.at[my_row], send0.at[step], recv0.at[my_row],
            device_id={"row": lax.rem(my_row + step, rows), "col": my_col},
            device_id_type=MESH,
        )

    def copy0_col(step):
        return pltpu.make_async_remote_copy(
            own, recv.at[rows + my_col], send0.at[rows + step], recv0.at[rows + my_col],
            device_id={"row": my_row, "col": lax.rem(my_col + step, cols)},
            device_id_type=MESH,
        )

    def each(first, last, action):
        def one(step, _):
            action(step)
            return 0

        lax.fori_loop(first, last, one, 0)

    each(rows // 2, rows, lambda s: copy0_row(s).start())
    each(1, rows // 2, lambda s: copy0_row(s).start())
    each(1, cols, lambda s: copy0_col(s).start())

    def landed0(slot):
        pltpu.make_async_remote_copy(
            own, recv.at[slot], send0.at[0], recv0.at[slot],
            device_id={"row": my_row, "col": my_col}, device_id_type=MESH,
        ).wait_recv()

    each(1, rows, lambda s: landed0(lax.rem(my_row + s, rows)))
    each(1, cols, lambda s: landed0(rows + lax.rem(my_col + s, cols)))

    def unpack(slot):
        for k in range(SENT):
            home = 7 if k == 4 else k
            for b in range(blk_dev):
                attr[home, pl.ds(slot * blk_dev + b, 1), :] = recv[slot, k * blk_dev + b]

    def unpack_all(slot, _):
        unpack(slot)
        return 0

    lax.fori_loop(0, rows + cols, unpack_all, 0)

    def by_type(row):
        kind = attr[7]
        value = jnp.full(kind.shape, table_ref[row, 0], jnp.float32)
        for t in range(1, types):
            value = jnp.where(kind == t, table_ref[row, t], value)
        return value

    rho = by_type(0)
    attr[4] = rho
    attr[5] = by_type(1) * rho * rho * rho
    attr[6] = by_type(2)

    sub = lax.broadcasted_iota(jnp.int32, (8, TILE), 0)

    def stack_columns(values):
        block = jnp.broadcast_to(values[0], (8, TILE))
        for k in range(1, len(values)):
            block = jnp.where(sub == k, jnp.broadcast_to(values[k], (8, TILE)), block)
        return block.T

    def fold(value):
        out = value[0:8]
        for s in range(8, STRIP, 8):
            out = out + value[s : s + 8]
        return out

    def wide(value):
        return jnp.broadcast_to(value, (STRIP, TILE))

    def tile_of(slot):
        first, second = tiles_ref[0, slot], tiles_ref[1, slot]
        return jnp.maximum(first, 0), jnp.maximum(second, 0), first

    def add_up(slot, first, sums):
        block, _, _ = tile_of(slot)
        for a in range(blocks_i):
            chosen = jnp.where(block == a, 1.0, 0.0)
            for k, value in enumerate(sums):
                acc[first + k, a] += chosen * value

    def row_of(k, block_i):
        return wide(attr[k, pl.ds(blocks_j + block_i, 1), :])

    strips = range(0, TILE, STRIP)
    row_ids = lax.broadcasted_iota(jnp.int32, (STRIP, TILE), 0)
    lane_ids = lax.broadcasted_iota(jnp.int32, (STRIP, TILE), 1)

    def born_sweep(slot, _):
        bi, bj, first = tile_of(slot)
        live = jnp.where(first >= 0, 1.0, 0.0)
        global_i = my_row * blocks_i + bi
        global_j = (lax.div(bj, blk_dev) * cols + my_col) * blk_dev + lax.rem(bj, blk_dev)
        self_pair = jnp.where(global_i == global_j, 1.0, 0.0)
        jcol[slot] = stack_columns([attr[k, pl.ds(bj, 1), :] for k in range(7)])
        xi, yi, zi = (row_of(k, bi) for k in range(3))
        rho_i = row_of(4, bi)
        rho_sq = rho_i * rho_i
        gap_i = rho_i + NECK_GAP
        born = jnp.zeros((8, TILE), jnp.float32)
        for s in strips:
            span = pl.ds(s, STRIP)
            col = lambda k: wide(jcol[slot, span, k : k + 1])
            dx, dy, dz = xi - col(0), yi - col(1), zi - col(2)
            q = dx * dx + dy * dy + dz * dz
            diagonal = jnp.where(row_ids + s == lane_ids, self_pair, 0.0)
            t = jnp.maximum((live - diagonal) - q * (1.0 / CUTOFF_SQ), 0.0)
            rho_j = col(4)
            inv = 1.0 / (q + rho_sq)
            gap = gap_i + rho_j
            off = q - gap * gap
            bump = jnp.exp2(off * off * (-LOG2E / NECK_WIDTH))
            born = born + fold(t * t * (col(5) * inv * inv + col(6) * bump))
            geo[0, slot, span, :] = dx
            geo[1, slot, span, :] = dy
            geo[2, slot, span, :] = dz
            geo[3, slot, span, :] = q
            geo[4, slot, span, :] = t
            geo[5, slot, span, :] = bump
        add_up(slot, 0, [born])
        return 0

    lax.fori_loop(0, slots, born_sweep, 0)

    def exchange(index, piece, landing, send, receive):
        for a in range(blocks_i):
            value = jnp.sum(acc[index, a], axis=0, keepdims=True)
            piece[a] = value
            landing[my_col, blocks_j + a] = value
        for b in range(blk_dev):
            landing[my_col, my_row * blk_dev + b] = piece[my_col * blk_dev + b]

        def copy_all(step):
            peer = lax.rem(me + step, devices)
            peer_row, peer_col = lax.div(peer, cols), lax.rem(peer, cols)
            return pltpu.make_async_remote_copy(
                piece.at[pl.ds(peer_col * blk_dev, blk_dev)],
                landing.at[my_col, pl.ds(my_row * blk_dev, blk_dev)],
                send.at[step], receive.at[me],
                device_id={"row": peer_row, "col": peer_col}, device_id_type=MESH,
            )

        def copy_col(step):
            return pltpu.make_async_remote_copy(
                piece, landing.at[my_col, pl.ds(blocks_j, blocks_i)],
                send.at[devices + step], receive.at[devices + my_col],
                device_id={"row": my_row, "col": lax.rem(my_col + step, cols)},
                device_id_type=MESH,
            )

        each(devices // 2, devices, lambda s: copy_all(s).start())
        each(1, devices // 2, lambda s: copy_all(s).start())
        each(1, cols, lambda s: copy_col(s).start())

        def finish():
            def landed(step):
                peer = lax.rem(me + step, devices)
                peer_row, peer_col = lax.div(peer, cols), lax.rem(peer, cols)
                pltpu.make_async_remote_copy(
                    piece.at[pl.ds(0, blk_dev)],
                    landing.at[peer_col, pl.ds(peer_row * blk_dev, blk_dev)],
                    send.at[0], receive.at[peer],
                    device_id={"row": my_row, "col": my_col}, device_id_type=MESH,
                ).wait_recv()

            def landed_col(step):
                peer_col = lax.rem(my_col + step, cols)
                pltpu.make_async_remote_copy(
                    piece, landing.at[peer_col, pl.ds(blocks_j, blocks_i)],
                    send.at[0], receive.at[devices + peer_col],
                    device_id={"row": my_row, "col": my_col}, device_id_type=MESH,
                ).wait_recv()

            each(1, devices, landed)
            each(1, cols, landed_col)
            for b in range(blocks_j + blocks_i):
                value = landing[0, b]
                for c in range(1, cols):
                    value = value + landing[c, b]
                total[pl.ds(b, 1), :] = value

        def drain():
            each(1, devices, lambda s: copy_all(s).wait_send())
            each(1, cols, lambda s: copy_col(s).wait_send())

        return finish, drain

    finish1, drain1 = exchange(0, part, partial_recv, send1, recv1)

    def slope_sweep(slot, _):
        bi, _, _ = tile_of(slot)
        rho_i, vol_i, neck_i = row_of(4, bi), row_of(5, bi), row_of(6, bi)
        rho_sq = rho_i * rho_i
        gap_i = rho_i + NECK_GAP
        sums = [jnp.zeros((8, TILE), jnp.float32) for _ in range(3)]
        for s in strips:
            span = pl.ds(s, STRIP)
            col = lambda k: wide(jcol[slot, span, k : k + 1])
            d = [geo[k, slot, span, :] for k in range(3)]
            q, t, bump = (geo[k, slot, span, :] for k in range(3, 6))
            rho_j = col(4)
            soft_i, soft_j = q + rho_sq, q + rho_j * rho_j
            both = 1.0 / (soft_i * soft_j)
            inv_i, inv_j = both * soft_j, both * soft_i
            gap = gap_i + rho_j
            off = (q - gap * gap) * (2.0 / NECK_WIDTH)

            def slope(volume, neck, inv):
                far = volume * inv * inv
                near = neck * bump
                return t * (t * (2.0 * far * inv + near * off) + (2.0 / CUTOFF_SQ) * (far + near))

            slope_ij = slope(col(5), col(6), inv_i)
            slope_ji = slope(vol_i, neck_i, inv_j)
            for k in range(3):
                sums[k] = sums[k] + fold(slope_ij * d[k])
                mom[k, slot, span, :] = slope_ji * d[k]
        add_up(slot, 1, sums)
        return 0

    lax.fori_loop(0, slots, slope_sweep, 0)
    alpha, beta, gamma = by_type(3), by_type(4), by_type(5)
    finish1()

    rho = attr[4]
    scaled = rho * total[...]
    squash = jnp.tanh(
        alpha * scaled - beta * scaled * scaled + gamma * scaled * scaled * scaled
    )
    rad = 1.0 / (1.0 / rho - squash / (rho + OFFSET))
    radius[0] = rad
    radius[1] = 1.0 / rad
    radius[2] = rad * attr[3]
    rate[...] = (
        rad * rad * (1.0 - squash * squash)
        * (alpha - 2.0 * beta * scaled + 3.0 * gamma * scaled * scaled)
        * rho / (rho + OFFSET)
    )

    def pair_sweep(slot, _):
        bi, bj, _ = tile_of(slot)
        jrad = stack_columns([radius[k, pl.ds(bj, 1), :] for k in range(3)])
        rad_i = wide(radius[0, pl.ds(blocks_j + bi, 1), :])
        quarter_i = wide(0.25 * radius[1, pl.ds(blocks_j + bi, 1), :])
        grad = jnp.zeros((8, TILE), jnp.float32)
        for s in strips:
            span = pl.ds(s, STRIP)
            col = lambda k: wide(jrad[s : s + STRIP, k : k + 1])
            q, t = geo[3, slot, span, :], geo[4, slot, span, :]
            ratio = q * quarter_i * col(1)
            decay = jnp.exp2(ratio * (-LOG2E))
            inv = lax.rsqrt(q + rad_i * col(0) * decay)
            lean = t * t * (inv * inv * inv)
            grad = grad + fold(lean * (decay + decay * ratio) * col(2))
            geo[5, slot, span, :] = t * (-2.0 / CUTOFF_SQ) * inv - 0.5 * lean * (1.0 - 0.25 * decay)
        add_up(slot, 4, [grad])
        return 0

    lax.fori_loop(0, slots, pair_sweep, 0)
    for a in range(blocks_i):
        acc[4, a] = acc[4, a] * (-0.5 * attr[3, pl.ds(blocks_j + a, 1), :])
    finish2, drain2 = exchange(4, grad_part, grad_recv, send2, recv2)

    def direct_sweep(slot, _):
        sums = [jnp.zeros((8, TILE), jnp.float32) for _ in range(3)]
        for s in strips:
            span = pl.ds(s, STRIP)
            pull = geo[5, slot, span, :] * wide(jcol[slot, span, 3:4])
            for k in range(3):
                sums[k] = sums[k] + fold(pull * geo[k, slot, span, :])
        add_up(slot, 5, sums)
        return 0

    lax.fori_loop(0, slots, direct_sweep, 0)
    finish2()

    charge = attr[3]
    rad = radius[0]
    chain[...] = (
        COULOMB * charge * charge / (2.0 * rad * rad) - COULOMB * total[...]
    ) * rate[...]

    def chain_sweep(slot, _):
        _, bj, _ = tile_of(slot)
        jchain = stack_columns([chain[pl.ds(bj, 1), :]])
        sums = [jnp.zeros((8, TILE), jnp.float32) for _ in range(3)]
        for s in strips:
            span = pl.ds(s, STRIP)
            factor = wide(jchain[s : s + STRIP, 0:1])
            for k in range(3):
                sums[k] = sums[k] + fold(factor * mom[k, slot, span, :])
        add_up(slot, 8, sums)
        return 0

    lax.fori_loop(0, slots, chain_sweep, 0)

    for a in range(blocks_i):
        home = pl.ds(blocks_j + a, 1)
        for k in range(3):
            direct = jnp.sum(acc[5 + k, a], axis=0, keepdims=True)
            own_chain = jnp.sum(acc[1 + k, a], axis=0, keepdims=True)
            other = jnp.sum(acc[8 + k, a], axis=0, keepdims=True)
            frc_part[a // blk_dev, k * blk_dev + a % blk_dev] = (
                2.0 * COULOMB * attr[3, home, :] * direct
                + 2.0 * (chain[home, :] * own_chain + other)
            )

    def copy3(step):
        peer_col = lax.rem(my_col + step, cols)
        return pltpu.make_async_remote_copy(
            frc_part.at[peer_col], frc_recv.at[my_col], send3.at[step], recv3.at[my_col],
            device_id={"row": my_row, "col": peer_col}, device_id_type=MESH,
        )

    def landed3(step):
        peer_col = lax.rem(my_col + step, cols)
        pltpu.make_async_remote_copy(
            frc_part.at[0], frc_recv.at[peer_col], send3.at[0], recv3.at[peer_col],
            device_id={"row": my_row, "col": my_col}, device_id_type=MESH,
        ).wait_recv()

    each(1, cols, lambda s: copy3(s).start())
    frc_recv[my_col] = frc_part[my_col]
    each(1, rows, lambda s: copy0_row(s).wait_send())
    each(1, cols, lambda s: copy0_col(s).wait_send())
    drain1()
    drain2()
    each(1, cols, landed3)
    for b in range(blk_dev):
        span = pl.ds(b * TILE, TILE)
        for k in range(3):
            value = frc_recv[0, k * blk_dev + b]
            for c in range(1, cols):
                value = value + frc_recv[c, k * blk_dev + b]
            frc_out[k : k + 1, span] = value
            vel_out[k : k + 1, span] = vel_ref[k : k + 1, span] + TIMESTEP / (2.0 * mass[b]) * (
                frc_ref[k : k + 1, span] + value
            )
    each(1, cols, lambda s: copy3(s).wait_send())


def solution(mesh):
    rows, cols = mesh.shape["row"], mesh.shape["col"]
    devices = rows * cols

    def body(positions, velocities, old_forces, charges, atom_types, type_table, tile_pairs):
        own_count = positions.shape[1]
        blk_dev = own_count // TILE
        slots = tile_pairs.shape[-1]
        blocks_i, blocks_j = cols * blk_dev, rows * blk_dev
        blocks = -(-(blocks_i + blocks_j) // 8) * 8
        vmem = pl.BlockSpec(memory_space=pltpu.VMEM)
        smem = pl.BlockSpec(memory_space=pltpu.SMEM)
        f32 = lambda *shape: pltpu.VMEM(shape, jnp.float32)
        dma = lambda n: pltpu.SemaphoreType.DMA((n,))
        result = jax.ShapeDtypeStruct(positions.shape, jnp.float32)
        return pl.pallas_call(
            functools.partial(kernel, rows, cols, blk_dev),
            out_shape=(result, result, result),
            in_specs=[smem, smem] + [vmem] * 5,
            out_specs=(vmem, vmem, vmem),
            scratch_shapes=[
                f32(SENT * blk_dev, 1, TILE),
                f32(rows + cols, SENT * blk_dev, 1, TILE),
                f32(8, blocks, TILE),
                f32(blocks, TILE),
                f32(3, blocks, TILE),
                f32(blocks, TILE),
                f32(blocks, TILE),
                f32(slots, TILE, 8),
                f32(6, slots, TILE, TILE),
                f32(3, slots, TILE, TILE),
                f32(11, blocks_i, 8, TILE),
                f32(blocks_i, 1, TILE),
                f32(cols, blocks_j + blocks_i, 1, TILE),
                f32(blocks_i, 1, TILE),
                f32(cols, blocks_j + blocks_i, 1, TILE),
                f32(cols, 3 * blk_dev, 1, TILE),
                f32(cols, 3 * blk_dev, 1, TILE),
                dma(rows + cols), dma(rows + cols),
                dma(devices + cols), dma(devices + cols),
                dma(devices + cols), dma(devices + cols),
                dma(cols), dma(cols),
            ],
            compiler_params=pltpu.CompilerParams(
                collective_id=0, has_side_effects=True, vmem_limit_bytes=40 * 1024 * 1024
            ),
            name="verlet",
        )(
            type_table, tile_pairs[0, 0], positions, velocities, old_forces,
            charges.reshape(blk_dev, TILE), atom_types.reshape(blk_dev, TILE),
        )

    return jax.shard_map(
        body,
        mesh=mesh,
        in_specs=(
            P(None, ("row", "col")),
            P(None, ("row", "col")),
            P(None, ("row", "col")),
            P(("row", "col")),
            P(("row", "col")),
            P(),
            P("row", "col", None, None),
        ),
        out_specs=(P(None, ("row", "col")), P(None, ("row", "col")), P(None, ("row", "col"))),
        check_vma=False,
    )
```

```python
import functools
import math

import jax
import jax.numpy as jnp
from jax import lax
from jax.experimental import pallas as pl
from jax.experimental.pallas import tpu as pltpu
from jax.sharding import PartitionSpec as P

TILE = 128
STRIP = 8
CUTOFF_SQ = 144.0
COULOMB = 32.0
TIMESTEP = 0.5
OFFSET = 0.09
NECK_GAP = 0.5
NECK_WIDTH = 16.0
LOG2E = math.log2(math.e)
MESH = pl.DeviceIdType.MESH
SENT = 5


def kernel(
    rows, cols, blk_dev, table_in, tiles_in, pos_in, vel_in, frc_in, chg_in, typ_in,
    out,
    table_ref, tiles_ref, pos_ref, vel_ref, frc_ref, chg_ref, typ_ref, load_sem,
    own, recv, attr, total, radius, rate, chain, turned, turned_rad, turned_chain, geo, mom, acc, part, partial_recv,
    grad_part, grad_recv, frc_part, frc_recv,
    send0, recv0, send1, recv1, send2, recv2, send3, recv3,
):
    my_row, my_col = lax.axis_index("row"), lax.axis_index("col")
    devices = rows * cols
    me = my_row * cols + my_col
    blocks_j, blocks_i = rows * blk_dev, cols * blk_dev
    slots = tiles_ref.shape[1]
    types = table_ref.shape[1]

    loads = [
        pltpu.make_async_copy(source, held, load_sem.at[k])
        for k, (source, held) in enumerate((
            (table_in, table_ref), (typ_in, typ_ref), (pos_in, pos_ref), (vel_in, vel_ref),
            (frc_in, frc_ref), (chg_in, chg_ref), (tiles_in.at[0, 0], tiles_ref),
        ))
    ]
    for load in loads:
        load.start()
    barrier = pltpu.get_barrier_semaphore()

    def greet(step, _):
        peer = lax.rem(me + step, devices)
        pl.semaphore_signal(
            barrier, inc=1,
            device_id={"row": lax.div(peer, cols), "col": lax.rem(peer, cols)},
            device_id_type=MESH,
        )
        return 0

    lax.fori_loop(1, devices, greet, 0)

    for load in loads:
        load.wait()

    mass = []
    for b in range(blk_dev):
        span = pl.ds(b * TILE, TILE)
        kind = typ_ref[b : b + 1, :].astype(jnp.float32)
        m = jnp.zeros((1, TILE), jnp.float32)
        for t in range(types):
            m = jnp.where(kind == t, table_ref[6, t], m)
        mass.append(m)
        for k in range(3):
            x = (
                pos_ref[k : k + 1, span]
                + TIMESTEP * vel_ref[k : k + 1, span]
                + TIMESTEP * TIMESTEP / (2.0 * m) * frc_ref[k : k + 1, span]
            )
            out[0, k : k + 1, span] = x
            own[k * blk_dev + b] = x
            recv[my_row, k * blk_dev + b] = x
            recv[rows + my_col, k * blk_dev + b] = x
        for k, value in ((3, chg_ref[b : b + 1, :]), (4, kind)):
            own[k * blk_dev + b] = value
            recv[my_row, k * blk_dev + b] = value
            recv[rows + my_col, k * blk_dev + b] = value
    acc[...] = jnp.zeros_like(acc)
    attr[...] = jnp.zeros_like(attr)
    total[...] = jnp.zeros_like(total)

    pl.semaphore_wait(barrier, devices - 1)

    def copy0_row(step):
        return pltpu.make_async_remote_copy(
            own, recv.at[my_row], send0.at[step], recv0.at[my_row],
            device_id={"row": lax.rem(my_row + step, rows), "col": my_col},
            device_id_type=MESH,
        )

    def copy0_col(step):
        return pltpu.make_async_remote_copy(
            own, recv.at[rows + my_col], send0.at[rows + step], recv0.at[rows + my_col],
            device_id={"row": my_row, "col": lax.rem(my_col + step, cols)},
            device_id_type=MESH,
        )

    def each(first, last, action):
        def one(step, _):
            action(step)
            return 0

        lax.fori_loop(first, last, one, 0)

    each(rows // 2, rows, lambda s: copy0_row(s).start())
    each(1, rows // 2, lambda s: copy0_row(s).start())
    each(1, cols, lambda s: copy0_col(s).start())

    def landed0(slot):
        pltpu.make_async_remote_copy(
            own, recv.at[slot], send0.at[0], recv0.at[slot],
            device_id={"row": my_row, "col": my_col}, device_id_type=MESH,
        ).wait_recv()

    each(1, rows, lambda s: landed0(lax.rem(my_row + s, rows)))
    each(1, cols, lambda s: landed0(rows + lax.rem(my_col + s, cols)))

    def unpack(slot):
        for k in range(SENT):
            home = 7 if k == 4 else k
            for b in range(blk_dev):
                attr[home, pl.ds(slot * blk_dev + b, 1), :] = recv[slot, k * blk_dev + b]

    def unpack_all(slot, _):
        unpack(slot)
        return 0

    lax.fori_loop(0, rows + cols, unpack_all, 0)

    def by_type(row):
        kind = attr[7]
        value = jnp.full(kind.shape, table_ref[row, 0], jnp.float32)
        for t in range(1, types):
            value = jnp.where(kind == t, table_ref[row, t], value)
        return value

    rho = by_type(0)
    attr[4] = rho
    attr[5] = by_type(1) * rho * rho * rho
    attr[6] = by_type(2)

    def turn(value):
        return pltpu.roll(wide(value), 0, 1, stride=1, stride_axis=0)

    def strip(base, s):
        return pltpu.roll(base, s, 1) if s else base

    def each_block(action):
        def some(step, _):
            for k in range(blk_dev):
                action(step * blk_dev + k)
            return 0

        lax.fori_loop(0, rows, some, 0)

    def each_tile(sweep):
        group = 2 if slots % 2 == 0 else 1

        def some(step, _):
            for k in range(group):
                sweep(step * group + k)
            return 0

        lax.fori_loop(0, slots // group, some, 0)

    def wide(value):
        return jnp.broadcast_to(value, (STRIP, TILE))

    def tile_of(slot):
        first, second = tiles_ref[0, slot], tiles_ref[1, slot]
        return jnp.maximum(first, 0), jnp.maximum(second, 0), first

    def add_up(slot, first, sums):
        block, _, _ = tile_of(slot)
        for a in range(blocks_i):
            chosen = jnp.where(block == a, 1.0, 0.0)
            for k, value in enumerate(sums):
                acc[first + k, a] += chosen * value

    def row_of(k, block_i):
        return wide(attr[k, pl.ds(blocks_j + block_i, 1), :])

    strips = range(0, TILE, STRIP)
    same_atom = jnp.where(lax.broadcasted_iota(jnp.int32, (STRIP, TILE), 0) == 0, 1.0, 0.0)

    def turn_attr(block):
        for k in range(7):
            turned[k, block] = turn(attr[k, pl.ds(block, 1), :])

    each_block(turn_attr)

    def born_sweep(slot):
        bi, bj, first = tile_of(slot)
        live = jnp.where(first >= 0, 1.0, 0.0)
        global_i = my_row * blocks_i + bi
        global_j = (lax.div(bj, blk_dev) * cols + my_col) * blk_dev + lax.rem(bj, blk_dev)
        self_pair = jnp.where(global_i == global_j, 1.0, 0.0)
        base = {k: turned[k, bj] for k in (0, 1, 2, 4, 5, 6)}
        xi, yi, zi = (row_of(k, bi) for k in range(3))
        rho_i = row_of(4, bi)
        rho_sq = rho_i * rho_i
        gap_i = rho_i + NECK_GAP
        born = jnp.zeros((8, TILE), jnp.float32)
        for s in strips:
            span = pl.ds(s, STRIP)
            col = lambda k: strip(base[k], s)
            dx, dy, dz = xi - col(0), yi - col(1), zi - col(2)
            q = dx * dx + dy * dy + dz * dz
            t = jnp.maximum((live if s else live - self_pair * same_atom) - q * (1.0 / CUTOFF_SQ), 0.0)
            rho_j = col(4)
            inv = 1.0 / (q + rho_sq)
            gap = gap_i + rho_j
            off = q - gap * gap
            bump = jnp.exp2(off * off * (-LOG2E / NECK_WIDTH))
            born = born + (t * t * (col(5) * inv * inv + col(6) * bump))
            geo[0, slot, span, :] = dx
            geo[1, slot, span, :] = dy
            geo[2, slot, span, :] = dz
            geo[3, slot, span, :] = q
            geo[4, slot, span, :] = t
            geo[5, slot, span, :] = bump
        add_up(slot, 0, [born])

    each_tile(born_sweep)

    def exchange(index, piece, landing, send, receive):
        for a in range(blocks_i):
            value = jnp.sum(acc[index, a], axis=0, keepdims=True)
            piece[a] = value
            landing[my_col, blocks_j + a] = value
        for b in range(blk_dev):
            landing[my_col, my_row * blk_dev + b] = piece[my_col * blk_dev + b]

        def copy_all(step):
            peer = lax.rem(me + step, devices)
            peer_row, peer_col = lax.div(peer, cols), lax.rem(peer, cols)
            return pltpu.make_async_remote_copy(
                piece.at[pl.ds(peer_col * blk_dev, blk_dev)],
                landing.at[my_col, pl.ds(my_row * blk_dev, blk_dev)],
                send.at[step], receive.at[me],
                device_id={"row": peer_row, "col": peer_col}, device_id_type=MESH,
            )

        def copy_col(step):
            return pltpu.make_async_remote_copy(
                piece, landing.at[my_col, pl.ds(blocks_j, blocks_i)],
                send.at[devices + step], receive.at[devices + my_col],
                device_id={"row": my_row, "col": lax.rem(my_col + step, cols)},
                device_id_type=MESH,
            )

        each(devices // 2, devices, lambda s: copy_all(s).start())
        each(1, devices // 2, lambda s: copy_all(s).start())
        each(1, cols, lambda s: copy_col(s).start())

        def finish():
            def landed(step):
                peer = lax.rem(me + step, devices)
                peer_row, peer_col = lax.div(peer, cols), lax.rem(peer, cols)
                pltpu.make_async_remote_copy(
                    piece.at[pl.ds(0, blk_dev)],
                    landing.at[peer_col, pl.ds(peer_row * blk_dev, blk_dev)],
                    send.at[0], receive.at[peer],
                    device_id={"row": my_row, "col": my_col}, device_id_type=MESH,
                ).wait_recv()

            def landed_col(step):
                peer_col = lax.rem(my_col + step, cols)
                pltpu.make_async_remote_copy(
                    piece, landing.at[peer_col, pl.ds(blocks_j, blocks_i)],
                    send.at[0], receive.at[devices + peer_col],
                    device_id={"row": my_row, "col": my_col}, device_id_type=MESH,
                ).wait_recv()

            each(1, devices, landed)
            each(1, cols, landed_col)
            for b in range(blocks_j + blocks_i):
                value = landing[0, b]
                for c in range(1, cols):
                    value = value + landing[c, b]
                total[pl.ds(b, 1), :] = value

        def drain():
            each(1, devices, lambda s: copy_all(s).wait_send())
            each(1, cols, lambda s: copy_col(s).wait_send())

        return finish, drain

    finish1, drain1 = exchange(0, part, partial_recv, send1, recv1)

    def slope_sweep(slot):
        bi, bj, _ = tile_of(slot)
        base = {k: turned[k, bj] for k in (4, 5, 6)}
        rho_i, vol_i, neck_i = row_of(4, bi), row_of(5, bi), row_of(6, bi)
        rho_sq = rho_i * rho_i
        gap_i = rho_i + NECK_GAP
        sums = [jnp.zeros((8, TILE), jnp.float32) for _ in range(3)]
        for s in strips:
            span = pl.ds(s, STRIP)
            col = lambda k: strip(base[k], s)
            d = [geo[k, slot, span, :] for k in range(3)]
            q, t, bump = (geo[k, slot, span, :] for k in range(3, 6))
            rho_j = col(4)
            soft_i, soft_j = q + rho_sq, q + rho_j * rho_j
            both = 1.0 / (soft_i * soft_j)
            inv_i, inv_j = both * soft_j, both * soft_i
            gap = gap_i + rho_j
            off = (q - gap * gap) * (2.0 / NECK_WIDTH)

            def slope(volume, neck, inv):
                far = volume * inv * inv
                near = neck * bump
                return t * (t * (2.0 * far * inv + near * off) + (2.0 / CUTOFF_SQ) * (far + near))

            slope_ij = slope(col(5), col(6), inv_i)
            slope_ji = slope(vol_i, neck_i, inv_j)
            for k in range(3):
                sums[k] = sums[k] + (slope_ij * d[k])
                mom[k, slot, span, :] = slope_ji * d[k]
        add_up(slot, 1, sums)

    each_tile(slope_sweep)
    alpha, beta, gamma = by_type(3), by_type(4), by_type(5)
    finish1()

    rho = attr[4]
    scaled = rho * total[...]
    squash = jnp.tanh(
        alpha * scaled - beta * scaled * scaled + gamma * scaled * scaled * scaled
    )
    rad = 1.0 / (1.0 / rho - squash / (rho + OFFSET))
    radius[0] = rad
    radius[1] = 1.0 / rad
    radius[2] = rad * attr[3]
    rate[...] = (
        rad * rad * (1.0 - squash * squash)
        * (alpha - 2.0 * beta * scaled + 3.0 * gamma * scaled * scaled)
        * rho / (rho + OFFSET)
    )

    def turn_radius(block):
        for k in range(3):
            turned_rad[k, block] = turn(radius[k, pl.ds(block, 1), :])

    each_block(turn_radius)

    def pair_sweep(slot):
        bi, bj, _ = tile_of(slot)
        base = [turned_rad[k, bj] for k in range(3)]
        rad_i = wide(radius[0, pl.ds(blocks_j + bi, 1), :])
        quarter_i = wide(0.25 * radius[1, pl.ds(blocks_j + bi, 1), :])
        grad = jnp.zeros((8, TILE), jnp.float32)
        for s in strips:
            span = pl.ds(s, STRIP)
            col = lambda k: strip(base[k], s)
            q, t = geo[3, slot, span, :], geo[4, slot, span, :]
            ratio = q * quarter_i * col(1)
            decay = jnp.exp2(ratio * (-LOG2E))
            inv = lax.rsqrt(q + rad_i * col(0) * decay)
            lean = t * t * (inv * inv * inv)
            grad = grad + (lean * (decay + decay * ratio) * col(2))
            geo[5, slot, span, :] = t * (-2.0 / CUTOFF_SQ) * inv - 0.5 * lean * (1.0 - 0.25 * decay)
        add_up(slot, 4, [grad])

    each_tile(pair_sweep)
    for a in range(blocks_i):
        acc[4, a] = acc[4, a] * (-0.5 * attr[3, pl.ds(blocks_j + a, 1), :])
    finish2, drain2 = exchange(4, grad_part, grad_recv, send2, recv2)

    def direct_sweep(slot):
        _, bj, _ = tile_of(slot)
        base = turned[3, bj]
        sums = [jnp.zeros((8, TILE), jnp.float32) for _ in range(3)]
        for s in strips:
            span = pl.ds(s, STRIP)
            pull = geo[5, slot, span, :] * strip(base, s)
            for k in range(3):
                sums[k] = sums[k] + (pull * geo[k, slot, span, :])
        add_up(slot, 5, sums)

    each_tile(direct_sweep)
    finish2()

    charge = attr[3]
    rad = radius[0]
    chain[...] = (
        COULOMB * charge * charge / (2.0 * rad * rad) - COULOMB * total[...]
    ) * rate[...]

    def turn_chain(block):
        turned_chain[block] = turn(chain[pl.ds(block, 1), :])

    each_block(turn_chain)

    def chain_sweep(slot):
        _, bj, _ = tile_of(slot)
        base = turned_chain[bj]
        sums = [jnp.zeros((8, TILE), jnp.float32) for _ in range(3)]
        for s in strips:
            span = pl.ds(s, STRIP)
            factor = strip(base, s)
            for k in range(3):
                sums[k] = sums[k] + (factor * mom[k, slot, span, :])
        add_up(slot, 8, sums)

    each_tile(chain_sweep)

    for a in range(blocks_i):
        home = pl.ds(blocks_j + a, 1)
        for k in range(3):
            direct = jnp.sum(acc[5 + k, a], axis=0, keepdims=True)
            own_chain = jnp.sum(acc[1 + k, a], axis=0, keepdims=True)
            other = jnp.sum(acc[8 + k, a], axis=0, keepdims=True)
            frc_part[a // blk_dev, k * blk_dev + a % blk_dev] = (
                2.0 * COULOMB * attr[3, home, :] * direct
                + 2.0 * (chain[home, :] * own_chain + other)
            )

    def copy3(step):
        peer_col = lax.rem(my_col + step, cols)
        return pltpu.make_async_remote_copy(
            frc_part.at[peer_col], frc_recv.at[my_col], send3.at[step], recv3.at[my_col],
            device_id={"row": my_row, "col": peer_col}, device_id_type=MESH,
        )

    def landed3(step):
        peer_col = lax.rem(my_col + step, cols)
        pltpu.make_async_remote_copy(
            frc_part.at[0], frc_recv.at[peer_col], send3.at[0], recv3.at[peer_col],
            device_id={"row": my_row, "col": my_col}, device_id_type=MESH,
        ).wait_recv()

    each(1, cols, lambda s: copy3(s).start())
    frc_recv[my_col] = frc_part[my_col]
    each(1, rows, lambda s: copy0_row(s).wait_send())
    each(1, cols, lambda s: copy0_col(s).wait_send())
    drain1()
    drain2()
    each(1, cols, landed3)
    for b in range(blk_dev):
        span = pl.ds(b * TILE, TILE)
        for k in range(3):
            value = frc_recv[0, k * blk_dev + b]
            for c in range(1, cols):
                value = value + frc_recv[c, k * blk_dev + b]
            out[1, k : k + 1, span] = value
            out[2, k : k + 1, span] = vel_ref[k : k + 1, span] + TIMESTEP / (2.0 * mass[b]) * (
                frc_ref[k : k + 1, span] + value
            )
    each(1, cols, lambda s: copy3(s).wait_send())


def solution(mesh):
    rows, cols = mesh.shape["row"], mesh.shape["col"]
    devices = rows * cols

    def body(positions, velocities, old_forces, charges, atom_types, type_table, tile_pairs):
        own_count = positions.shape[1]
        blk_dev = own_count // TILE
        slots = tile_pairs.shape[-1]
        blocks_i, blocks_j = cols * blk_dev, rows * blk_dev
        blocks = -(-(blocks_i + blocks_j) // 8) * 8
        vmem = pl.BlockSpec(memory_space=pltpu.VMEM)
        anywhere = pl.BlockSpec(memory_space=pl.ANY)
        f32 = lambda *shape: pltpu.VMEM(shape, jnp.float32)
        dma = lambda n: pltpu.SemaphoreType.DMA((n,))
        result = jax.ShapeDtypeStruct((3,) + positions.shape, jnp.float32)
        out = pl.pallas_call(
            functools.partial(kernel, rows, cols, blk_dev),
            out_shape=result,
            in_specs=[anywhere] * 7,
            out_specs=vmem,
            scratch_shapes=[
                pltpu.SMEM(type_table.shape, jnp.float32),
                pltpu.SMEM(tile_pairs.shape[2:], jnp.int32),
                f32(*positions.shape), f32(*positions.shape), f32(*positions.shape),
                f32(blk_dev, TILE),
                pltpu.VMEM((blk_dev, TILE), jnp.int32),
                dma(7),
                f32(SENT * blk_dev, 1, TILE),
                f32(rows + cols, SENT * blk_dev, 1, TILE),
                f32(8, blocks, TILE),
                f32(blocks, TILE),
                f32(3, blocks, TILE),
                f32(blocks, TILE),
                f32(blocks, TILE),
                f32(7, blocks_j, 8, TILE),
                f32(3, blocks_j, 8, TILE),
                f32(blocks_j, 8, TILE),
                f32(6, slots, TILE, TILE),
                f32(3, slots, TILE, TILE),
                f32(11, blocks_i, 8, TILE),
                f32(blocks_i, 1, TILE),
                f32(cols, blocks_j + blocks_i, 1, TILE),
                f32(blocks_i, 1, TILE),
                f32(cols, blocks_j + blocks_i, 1, TILE),
                f32(cols, 3 * blk_dev, 1, TILE),
                f32(cols, 3 * blk_dev, 1, TILE),
                dma(rows + cols), dma(rows + cols),
                dma(devices + cols), dma(devices + cols),
                dma(devices + cols), dma(devices + cols),
                dma(cols), dma(cols),
            ],
            compiler_params=pltpu.CompilerParams(
                collective_id=0, has_side_effects=True, vmem_limit_bytes=60000 * 1024
            ),
            name="verlet",
        )(
            type_table, tile_pairs, positions, velocities, old_forces,
            charges.reshape(blk_dev, TILE), atom_types.reshape(blk_dev, TILE),
        )
        return out[0], out[2], out[1]

    return jax.shard_map(
        body,
        mesh=mesh,
        in_specs=(
            P(None, ("row", "col")),
            P(None, ("row", "col")),
            P(None, ("row", "col")),
            P(("row", "col")),
            P(("row", "col")),
            P(),
            P("row", "col", None, None),
        ),
        out_specs=(P(None, ("row", "col")), P(None, ("row", "col")), P(None, ("row", "col"))),
        check_vma=False,
    )
```

```python
import functools
import math

import jax
import jax.numpy as jnp
from jax import lax
from jax.experimental import pallas as pl
from jax.experimental.pallas import tpu as pltpu
from jax.sharding import PartitionSpec as P

TILE = 128
STRIP = 8
CUTOFF_SQ = 144.0
COULOMB = 32.0
TIMESTEP = 0.5
OFFSET = 0.09
NECK_GAP = 0.5
NECK_WIDTH = 16.0
LOG2E = math.log2(math.e)
MESH = pl.DeviceIdType.MESH
SENT = 5


def kernel(
    rows, cols, blk_dev, table_in, tiles_in, pos_in, vel_in, frc_in, chg_in, typ_in,
    out,
    table_ref, tiles_ref, pos_ref, vel_ref, frc_ref, chg_ref, typ_ref, load_sem,
    own, recv, attr, total, radius, rate, chain, turned, turned_rad, geo, mom, acc, part, partial_recv,
    grad_part, grad_recv, frc_part, frc_recv,
    send0, recv0, send1, recv1, send2, recv2, send3, recv3,
):
    my_row, my_col = lax.axis_index("row"), lax.axis_index("col")
    devices = rows * cols
    me = my_row * cols + my_col
    blocks_j, blocks_i = rows * blk_dev, cols * blk_dev
    slots = tiles_ref.shape[1]
    types = table_ref.shape[1]

    loads = [
        pltpu.make_async_copy(source, held, load_sem.at[k])
        for k, (source, held) in enumerate((
            (table_in, table_ref), (typ_in, typ_ref), (pos_in, pos_ref), (vel_in, vel_ref),
            (frc_in, frc_ref), (chg_in, chg_ref), (tiles_in.at[0, 0], tiles_ref),
        ))
    ]
    for load in loads:
        load.start()
    barrier = pltpu.get_barrier_semaphore()

    def greet_row(step, _):
        pl.semaphore_signal(
            barrier, inc=1,
            device_id={"row": lax.rem(my_row + step, rows), "col": my_col},
            device_id_type=MESH,
        )
        return 0

    def greet_col(step, _):
        pl.semaphore_signal(
            barrier, inc=1,
            device_id={"row": my_row, "col": lax.rem(my_col + step, cols)},
            device_id_type=MESH,
        )
        return 0

    lax.fori_loop(1, rows, greet_row, 0)
    lax.fori_loop(1, cols, greet_col, 0)

    for load in loads:
        load.wait()

    mass = []
    for b in range(blk_dev):
        span = pl.ds(b * TILE, TILE)
        kind = typ_ref[b : b + 1, :].astype(jnp.float32)
        m = jnp.zeros((1, TILE), jnp.float32)
        for t in range(types):
            m = jnp.where(kind == t, table_ref[6, t], m)
        mass.append(m)
        for k in range(3):
            x = (
                pos_ref[k : k + 1, span]
                + TIMESTEP * vel_ref[k : k + 1, span]
                + TIMESTEP * TIMESTEP / (2.0 * m) * frc_ref[k : k + 1, span]
            )
            out[0, k : k + 1, span] = x
            own[k * blk_dev + b] = x
            recv[my_row, k * blk_dev + b] = x
            recv[rows + my_col, k * blk_dev + b] = x
        for k, value in ((3, chg_ref[b : b + 1, :]), (4, kind)):
            own[k * blk_dev + b] = value
            recv[my_row, k * blk_dev + b] = value
            recv[rows + my_col, k * blk_dev + b] = value
    acc[...] = jnp.zeros_like(acc)
    attr[...] = jnp.zeros_like(attr)
    total[...] = jnp.zeros_like(total)

    pl.semaphore_wait(barrier, rows + cols - 2)

    def copy0_row(step):
        return pltpu.make_async_remote_copy(
            own, recv.at[my_row], send0.at[step], recv0.at[my_row],
            device_id={"row": lax.rem(my_row + step, rows), "col": my_col},
            device_id_type=MESH,
        )

    def copy0_col(step):
        return pltpu.make_async_remote_copy(
            own, recv.at[rows + my_col], send0.at[rows + step], recv0.at[rows + my_col],
            device_id={"row": my_row, "col": lax.rem(my_col + step, cols)},
            device_id_type=MESH,
        )

    def each(first, last, action):
        def one(step, _):
            action(step)
            return 0

        lax.fori_loop(first, last, one, 0)

    each(rows // 2, rows, lambda s: copy0_row(s).start())
    each(1, rows // 2, lambda s: copy0_row(s).start())
    each(1, cols, lambda s: copy0_col(s).start())

    def landed0(slot):
        pltpu.make_async_remote_copy(
            own, recv.at[slot], send0.at[0], recv0.at[slot],
            device_id={"row": my_row, "col": my_col}, device_id_type=MESH,
        ).wait_recv()

    each(1, rows, lambda s: landed0(lax.rem(my_row + s, rows)))
    each(1, cols, lambda s: landed0(rows + lax.rem(my_col + s, cols)))

    def unpack(slot):
        for k in range(SENT):
            home = 7 if k == 4 else k
            for b in range(blk_dev):
                attr[home, pl.ds(slot * blk_dev + b, 1), :] = recv[slot, k * blk_dev + b]

    def unpack_all(slot, _):
        unpack(slot)
        return 0

    lax.fori_loop(0, rows + cols, unpack_all, 0)

    def by_type(row):
        kind = attr[7]
        value = jnp.full(kind.shape, table_ref[row, 0], jnp.float32)
        for t in range(1, types):
            value = jnp.where(kind == t, table_ref[row, t], value)
        return value

    rho = by_type(0)
    attr[4] = rho
    attr[5] = by_type(1) * rho * rho * rho
    attr[6] = by_type(2)

    def turn(value):
        return pltpu.roll(wide(value), 0, 1, stride=1, stride_axis=0)

    def strip(base, s):
        return pltpu.roll(base, s, 1) if s else base

    def back(value, s):
        return pltpu.roll(value, TILE - s, 1) if s else value

    def gather_up(value):
        level = value[0:1]
        for r in range(1, STRIP):
            level = level + back(value[r : r + 1], r)
        return level

    def each_tile(sweep):
        group = 2 if slots % 2 == 0 else 1

        def some(step, _):
            for k in range(group):
                sweep(step * group + k)
            return 0

        lax.fori_loop(0, slots // group, some, 0)

    def wide(value):
        return jnp.broadcast_to(value, (STRIP, TILE))

    def tile_of(slot):
        first, second = tiles_ref[0, slot], tiles_ref[1, slot]
        return jnp.maximum(first, 0), jnp.maximum(second, 0), first

    def add_up(slot, first, sums):
        block, _, _ = tile_of(slot)
        for a in range(blocks_i):
            chosen = jnp.where(block == a, 1.0, 0.0)
            for k, value in enumerate(sums):
                acc[first + k, a] += chosen * value

    def row_of(k, block_j):
        return wide(attr[k, pl.ds(block_j, 1), :])

    strips = range(0, TILE, STRIP)
    same_atom = jnp.where(lax.broadcasted_iota(jnp.int32, (STRIP, TILE), 0) == 0, 1.0, 0.0)

    def turn_strips(source, held, kinds):
        for a in range(blocks_i):
            for n, k in enumerate(kinds):
                base = turn(source[k, blocks_j + a : blocks_j + a + 1, :])
                for s in strips:
                    held[n, a, s // STRIP] = strip(base, s)

    turn_strips(attr, turned, (0, 1, 2, 4, 5, 6))

    def born_sweep(slot):
        bi, bj, first = tile_of(slot)
        live = jnp.where(first >= 0, 1.0, 0.0)
        global_i = my_row * blocks_i + bi
        global_j = (lax.div(bj, blk_dev) * cols + my_col) * blk_dev + lax.rem(bj, blk_dev)
        self_pair = jnp.where(global_i == global_j, 1.0, 0.0)
        xj, yj, zj, rho_j, vol_j, neck_j = (row_of(k, bj) for k in (0, 1, 2, 4, 5, 6))
        gap_j = rho_j + NECK_GAP
        born = jnp.zeros((8, TILE), jnp.float32)
        for s in strips:
            span = pl.ds(s, STRIP)
            own_i = lambda k: turned[k, bi, s // STRIP]
            dx, dy, dz = own_i(0) - xj, own_i(1) - yj, own_i(2) - zj
            q = dx * dx + dy * dy + dz * dz
            t = jnp.maximum((live if s else live - self_pair * same_atom) - q * (1.0 / CUTOFF_SQ), 0.0)
            rho_i = own_i(3)
            inv = 1.0 / (q + rho_i * rho_i)
            gap = rho_i + gap_j
            off = q - gap * gap
            bump = jnp.exp2(off * off * (-LOG2E / NECK_WIDTH))
            born = born + back(t * t * (vol_j * inv * inv + neck_j * bump), s)
            geo[0, slot, span, :] = dx
            geo[1, slot, span, :] = dy
            geo[2, slot, span, :] = dz
            geo[3, slot, span, :] = q
            geo[4, slot, span, :] = t
            geo[5, slot, span, :] = bump
        add_up(slot, 0, [born])

    each_tile(born_sweep)

    def exchange(index, scale, piece, landing, send, receive):
        for a in range(blocks_i):
            value = gather_up(acc[index, a]) * scale(a)
            piece[a] = value
            landing[my_col, blocks_j + a] = value
        for b in range(blk_dev):
            landing[my_col, my_row * blk_dev + b] = piece[my_col * blk_dev + b]

        def copy_all(step):
            peer = lax.rem(me + step, devices)
            peer_row, peer_col = lax.div(peer, cols), lax.rem(peer, cols)
            return pltpu.make_async_remote_copy(
                piece.at[pl.ds(peer_col * blk_dev, blk_dev)],
                landing.at[my_col, pl.ds(my_row * blk_dev, blk_dev)],
                send.at[step], receive.at[me],
                device_id={"row": peer_row, "col": peer_col}, device_id_type=MESH,
            )

        def copy_col(step):
            return pltpu.make_async_remote_copy(
                piece, landing.at[my_col, pl.ds(blocks_j, blocks_i)],
                send.at[devices + step], receive.at[devices + my_col],
                device_id={"row": my_row, "col": lax.rem(my_col + step, cols)},
                device_id_type=MESH,
            )

        each(devices // 2, devices, lambda s: copy_all(s).start())
        each(1, devices // 2, lambda s: copy_all(s).start())
        each(1, cols, lambda s: copy_col(s).start())

        def finish():
            def landed(step):
                peer = lax.rem(me + step, devices)
                peer_row, peer_col = lax.div(peer, cols), lax.rem(peer, cols)
                pltpu.make_async_remote_copy(
                    piece.at[pl.ds(0, blk_dev)],
                    landing.at[peer_col, pl.ds(peer_row * blk_dev, blk_dev)],
                    send.at[0], receive.at[peer],
                    device_id={"row": my_row, "col": my_col}, device_id_type=MESH,
                ).wait_recv()

            def landed_col(step):
                peer_col = lax.rem(my_col + step, cols)
                pltpu.make_async_remote_copy(
                    piece, landing.at[peer_col, pl.ds(blocks_j, blocks_i)],
                    send.at[0], receive.at[devices + peer_col],
                    device_id={"row": my_row, "col": my_col}, device_id_type=MESH,
                ).wait_recv()

            each(1, devices, landed)
            each(1, cols, landed_col)
            for b in range(blocks_j + blocks_i):
                value = landing[0, b]
                for c in range(1, cols):
                    value = value + landing[c, b]
                total[pl.ds(b, 1), :] = value

        def drain():
            each(1, devices, lambda s: copy_all(s).wait_send())
            each(1, cols, lambda s: copy_col(s).wait_send())

        return finish, drain

    finish1, drain1 = exchange(0, lambda a: 1.0, part, partial_recv, send1, recv1)

    def slope_sweep(slot):
        bi, bj, _ = tile_of(slot)
        rho_j, vol_j, neck_j = (row_of(k, bj) for k in (4, 5, 6))
        rho_sq = rho_j * rho_j
        gap_j = rho_j + NECK_GAP
        sums = [jnp.zeros((8, TILE), jnp.float32) for _ in range(3)]
        for s in strips:
            span = pl.ds(s, STRIP)
            rho_i, vol_i, neck_i = (turned[k, bi, s // STRIP] for k in range(3, 6))
            d = [geo[k, slot, span, :] for k in range(3)]
            q, t, bump = (geo[k, slot, span, :] for k in range(3, 6))
            soft_i, soft_j = q + rho_i * rho_i, q + rho_sq
            both = 1.0 / (soft_i * soft_j)
            inv_i, inv_j = both * soft_j, both * soft_i
            gap = rho_i + gap_j
            off = (q - gap * gap) * (2.0 / NECK_WIDTH)

            def slope(volume, neck, inv):
                far = volume * inv * inv
                near = neck * bump
                return t * (t * (2.0 * far * inv + near * off) + (2.0 / CUTOFF_SQ) * (far + near))

            slope_ij = slope(vol_j, neck_j, inv_i)
            slope_ji = slope(vol_i, neck_i, inv_j)
            for k in range(3):
                sums[k] = sums[k] + back(slope_ij * d[k], s)
                mom[k, slot, span, :] = back(slope_ji * d[k], s)
        add_up(slot, 1, sums)

    each_tile(slope_sweep)
    alpha, beta, gamma = by_type(3), by_type(4), by_type(5)
    finish1()

    rho = attr[4]
    scaled = rho * total[...]
    squash = jnp.tanh(
        alpha * scaled - beta * scaled * scaled + gamma * scaled * scaled * scaled
    )
    rad = 1.0 / (1.0 / rho - squash / (rho + OFFSET))
    radius[0] = rad
    radius[1] = 1.0 / rad
    radius[2] = rad * attr[3]
    rate[...] = (
        rad * rad * (1.0 - squash * squash)
        * (alpha - 2.0 * beta * scaled + 3.0 * gamma * scaled * scaled)
        * rho / (rho + OFFSET)
    )

    turn_strips(radius, turned_rad, (0, 1))

    def pair_sweep(slot):
        bi, bj, _ = tile_of(slot)
        rad_j, over_j, rad_charge_j = (wide(radius[k, pl.ds(bj, 1), :]) for k in range(3))
        quarter_j = 0.25 * over_j
        grad = jnp.zeros((8, TILE), jnp.float32)
        for s in strips:
            span = pl.ds(s, STRIP)
            q, t = geo[3, slot, span, :], geo[4, slot, span, :]
            ratio = q * (turned_rad[1, bi, s // STRIP] * quarter_j)
            decay = jnp.exp2(ratio * (-LOG2E))
            inv = lax.rsqrt(q + turned_rad[0, bi, s // STRIP] * rad_j * decay)
            lean = t * t * (inv * inv * inv)
            grad = grad + back(lean * (decay + decay * ratio) * rad_charge_j, s)
            geo[5, slot, span, :] = t * (-2.0 / CUTOFF_SQ) * inv - 0.5 * lean * (1.0 - 0.25 * decay)
        add_up(slot, 4, [grad])

    each_tile(pair_sweep)
    finish2, drain2 = exchange(
        4, lambda a: -0.5 * attr[3, blocks_j + a : blocks_j + a + 1, :], grad_part, grad_recv, send2, recv2
    )

    def direct_sweep(slot):
        _, bj, _ = tile_of(slot)
        charge_j = row_of(3, bj)
        sums = [jnp.zeros((8, TILE), jnp.float32) for _ in range(3)]
        for s in strips:
            span = pl.ds(s, STRIP)
            pull = geo[5, slot, span, :] * charge_j
            for k in range(3):
                sums[k] = sums[k] + back(pull * geo[k, slot, span, :], s)
        add_up(slot, 5, sums)

    each_tile(direct_sweep)
    finish2()

    charge = attr[3]
    rad = radius[0]
    chain[...] = (
        COULOMB * charge * charge / (2.0 * rad * rad) - COULOMB * total[...]
    ) * rate[...]

    def chain_sweep(slot):
        _, bj, _ = tile_of(slot)
        base = wide(chain[pl.ds(bj, 1), :])
        sums = [jnp.zeros((8, TILE), jnp.float32) for _ in range(3)]
        for s in strips:
            span = pl.ds(s, STRIP)
            factor = back(base, s)
            for k in range(3):
                sums[k] = sums[k] + (factor * mom[k, slot, span, :])
        add_up(slot, 8, sums)

    each_tile(chain_sweep)

    for a in range(blocks_i):
        home = pl.ds(blocks_j + a, 1)
        charge_i, chain_i = turn(attr[3, home, :]), turn(chain[home, :])
        for k in range(3):
            frc_part[a // blk_dev, k * blk_dev + a % blk_dev] = gather_up(
                2.0 * COULOMB * charge_i * acc[5 + k, a]
                + 2.0 * (chain_i * acc[1 + k, a] + acc[8 + k, a])
            )

    def copy3(step):
        peer_col = lax.rem(my_col + step, cols)
        return pltpu.make_async_remote_copy(
            frc_part.at[peer_col], frc_recv.at[my_col], send3.at[step], recv3.at[my_col],
            device_id={"row": my_row, "col": peer_col}, device_id_type=MESH,
        )

    def landed3(step):
        peer_col = lax.rem(my_col + step, cols)
        pltpu.make_async_remote_copy(
            frc_part.at[0], frc_recv.at[peer_col], send3.at[0], recv3.at[peer_col],
            device_id={"row": my_row, "col": my_col}, device_id_type=MESH,
        ).wait_recv()

    each(1, cols, lambda s: copy3(s).start())
    frc_recv[my_col] = frc_part[my_col]
    each(1, rows, lambda s: copy0_row(s).wait_send())
    each(1, cols, lambda s: copy0_col(s).wait_send())
    drain1()
    drain2()
    each(1, cols, landed3)
    for b in range(blk_dev):
        span = pl.ds(b * TILE, TILE)
        for k in range(3):
            value = frc_recv[0, k * blk_dev + b]
            for c in range(1, cols):
                value = value + frc_recv[c, k * blk_dev + b]
            out[1, k : k + 1, span] = value
            out[2, k : k + 1, span] = vel_ref[k : k + 1, span] + TIMESTEP / (2.0 * mass[b]) * (
                frc_ref[k : k + 1, span] + value
            )
    each(1, cols, lambda s: copy3(s).wait_send())


def solution(mesh):
    rows, cols = mesh.shape["row"], mesh.shape["col"]
    devices = rows * cols

    def body(positions, velocities, old_forces, charges, atom_types, type_table, tile_pairs):
        own_count = positions.shape[1]
        blk_dev = own_count // TILE
        slots = tile_pairs.shape[-1]
        blocks_i, blocks_j = cols * blk_dev, rows * blk_dev
        blocks = -(-(blocks_i + blocks_j) // 8) * 8
        vmem = pl.BlockSpec(memory_space=pltpu.VMEM)
        anywhere = pl.BlockSpec(memory_space=pl.ANY)
        f32 = lambda *shape: pltpu.VMEM(shape, jnp.float32)
        dma = lambda n: pltpu.SemaphoreType.DMA((n,))
        result = jax.ShapeDtypeStruct((3,) + positions.shape, jnp.float32)
        out = pl.pallas_call(
            functools.partial(kernel, rows, cols, blk_dev),
            out_shape=result,
            in_specs=[anywhere] * 7,
            out_specs=vmem,
            scratch_shapes=[
                pltpu.SMEM(type_table.shape, jnp.float32),
                pltpu.SMEM(tile_pairs.shape[2:], jnp.int32),
                f32(*positions.shape), f32(*positions.shape), f32(*positions.shape),
                f32(blk_dev, TILE),
                pltpu.VMEM((blk_dev, TILE), jnp.int32),
                dma(7),
                f32(SENT * blk_dev, 1, TILE),
                f32(rows + cols, SENT * blk_dev, 1, TILE),
                f32(8, blocks, TILE),
                f32(blocks, TILE),
                f32(3, blocks, TILE),
                f32(blocks, TILE),
                f32(blocks, TILE),
                f32(6, blocks_i, TILE // STRIP, STRIP, TILE),
                f32(2, blocks_i, TILE // STRIP, STRIP, TILE),
                f32(6, slots, TILE, TILE),
                f32(3, slots, TILE, TILE),
                f32(11, blocks_i, 8, TILE),
                f32(blocks_i, 1, TILE),
                f32(cols, blocks_j + blocks_i, 1, TILE),
                f32(blocks_i, 1, TILE),
                f32(cols, blocks_j + blocks_i, 1, TILE),
                f32(cols, 3 * blk_dev, 1, TILE),
                f32(cols, 3 * blk_dev, 1, TILE),
                dma(rows + cols), dma(rows + cols),
                dma(devices + cols), dma(devices + cols),
                dma(devices + cols), dma(devices + cols),
                dma(cols), dma(cols),
            ],
            compiler_params=pltpu.CompilerParams(
                collective_id=0, has_side_effects=True, vmem_limit_bytes=60000 * 1024
            ),
            name="verlet",
        )(
            type_table, tile_pairs, positions, velocities, old_forces,
            charges.reshape(blk_dev, TILE), atom_types.reshape(blk_dev, TILE),
        )
        return out[0], out[2], out[1]

    return jax.shard_map(
        body,
        mesh=mesh,
        in_specs=(
            P(None, ("row", "col")),
            P(None, ("row", "col")),
            P(None, ("row", "col")),
            P(("row", "col")),
            P(("row", "col")),
            P(),
            P("row", "col", None, None),
        ),
        out_specs=(P(None, ("row", "col")), P(None, ("row", "col")), P(None, ("row", "col"))),
        check_vma=False,
    )
```
